128 devices in a mesh: gx: 8 (over z_lo, y), gy: 16 (over z_hi, x, core).
Axes of the slice: x: 4, y: 4, z: 4 (z_hi: 2, z_lo: 2; z = z_hi * 2 + z_lo), core: 2. Of those that a mesh axis runs over, the one named last changes fastest.
Arguments:
- density_one: float32 [512, 512, 512], P('gx', 'gy'), may hold values from -6 to 6
- density_two: float32 [512, 512, 512], P('gx', 'gy'), may hold values from -6 to 6
Outputs:
- correlation: float32 [512, 512, 512], P('gx', 'gy')
The draws below stay inside these ranges and needn't reach their ends.
All inputs are finite; a program needn't handle non-finite values.
Results may differ from the reference program's by a relative error of at most 0.00013.
Values sent between devices are 32-bit elements; how exact they have to be, the bound alone decides.
A program may use at most 192 MiB of HBM per device.

```python
import math
import jax
import jax.numpy as jnp

NX = 512
NY = 512
NZ = 512


def levels(stream_key, extent, pieces, low, largest):
    def one(position, parts):
        steps = jax.random.uniform(jax.random.fold_in(jax.random.fold_in(stream_key, 6), position), (parts,), jnp.float32, low / len(pieces), largest / len(pieces))
        return jnp.repeat(jnp.exp(steps), extent[position] // parts).reshape((-1,) + (1,) * (len(extent) - position - 1))

    level = one(*pieces[0])
    for cut in pieces[1:]:
        level = level * one(*cut)
    return level


def normal_values(own_key, extent, scale, reach, cuts=(), kind=jnp.bfloat16):
    result = scale * jax.random.normal(own_key, extent, jnp.float32)
    if cuts:
        result = result * levels(own_key, extent, cuts, -0.22, 0.18)
    return jnp.clip(result, -reach, reach).astype(kind)


def setup_inputs(seed: int = 0) -> dict:
    arg_keys = jax.random.split(jax.random.key(seed), 3)
    return {
        "density_one": normal_values(arg_keys[0], (NX, NY, NZ), 1.0, 6.0, ((0, 8), (1, 16)), jnp.float32),
        "density_two": normal_values(arg_keys[1], (NX, NY, NZ), 1.0, 6.0, ((0, 8), (1, 16)), jnp.float32),
    }


def reference(density_one, density_two):
    cell_total = NX * NY * NZ
    spectrum_one = jnp.fft.rfftn(density_one)
    spectrum_two = jnp.fft.rfftn(density_two)
    power = (spectrum_one.real * spectrum_two.real + spectrum_one.imag * spectrum_two.imag) / cell_total
    wave_x = jnp.arange(NX)[:, None, None]
    wave_y = jnp.arange(NY)[None, :, None]
    wave_z = jnp.arange(NZ // 2 + 1)[None, None, :]
    kept_modes = (wave_x != NX // 2) & (wave_y != NY // 2) & (wave_z != NZ // 2)
    power = jnp.where(kept_modes, power, jnp.zeros_like(power))
    correlation = jnp.fft.irfftn(power * (1.0 + 0j), s=(NX, NY, NZ)) * math.sqrt(cell_total)
    return correlation.astype(jnp.float32)
```

```python
import functools
import math

import jax
import jax.numpy as jnp
import ml_dtypes
import numpy as np
from jax import lax
from jax.experimental import pallas as pl
from jax.experimental.pallas import tpu as pltpu
from jax.sharding import PartitionSpec as P

MESH = pl.DeviceIdType.MESH
NT = (((1,), (1,)), ((), ()))
NN = (((1,), (0,)), ((), ()))

GX, GY = 8, 16
PEERS = GX * GY
SIDE = 512
FWD_ROWS = 64
FWD_PITCH = 72
BACK_ROWS = 32
BACK_PITCH = 40
STEP = 45


def halves(table):
    high = table.astype(np.float32).astype(ml_dtypes.bfloat16)
    low = (table - high.astype(np.float64)).astype(np.float32).astype(ml_dtypes.bfloat16)
    return high, low


def wave(numerator, length):
    angle = 2.0 * np.pi * (numerator % length) / length
    return np.cos(angle), np.sin(angle)


def depth_table():
    kz = np.arange(SIDE // 2).reshape(2, PEERS)
    cos, sin = wave(kz[:, :, None] * np.arange(SIDE)[None, None, :], SIDE)
    return np.concatenate([cos, -sin], axis=1)


def plane_tables():
    m = np.arange(128)
    cos, sin = wave(m[:, None] * m[None, :], 128)
    rows_forward = np.block([[cos, sin], [-sin, cos]])
    rows_inverse = np.block([[cos, -sin], [sin, cos]])
    x4, y32 = m // 32, m % 32
    cos, sin = wave(
        128 * x4[:, None] * x4[None, :] + 16 * y32[:, None] * y32[None, :], SIDE
    )
    lanes_forward = np.block([[cos, -sin], [sin, cos]])
    lanes_inverse = np.concatenate([cos, sin], axis=1)
    parts = []
    for table in (rows_forward, rows_inverse, lanes_forward, lanes_inverse):
        parts.extend(halves(table))
    return np.concatenate(parts, axis=0)


def twiddle_factors():
    m = np.arange(128)
    x4, y32 = m // 32, m % 32
    x_cos, x_sin = wave(m[:, None] * x4[None, :], SIDE)
    y_cos, y_sin = wave(np.arange(16)[:, None] * y32[None, :], SIDE)
    return np.concatenate([x_cos, -x_sin, y_cos, -y_sin], axis=0).astype(np.float32)


def split(value):
    high = value.astype(jnp.bfloat16)
    low = (value - high.astype(jnp.float32)).astype(jnp.bfloat16)
    return high, low


def dot3(left, right, dims):
    def one(a, b):
        return lax.dot_general(a, b, dims, preferred_element_type=jnp.float32)

    return one(left[0], right[0]) + (one(left[0], right[1]) + one(left[1], right[0]))


def times(value, factor):
    if factor is None:
        return value
    (re, im), (c, s) = value, factor
    return (re * c - im * s, re * s + im * c)


def fourier4(v, sign):
    def add(p, q):
        return (p[0] + q[0], p[1] + q[1])

    def sub(p, q):
        return (p[0] - q[0], p[1] - q[1])

    s0, d0 = add(v[0], v[2]), sub(v[0], v[2])
    s1, d1 = add(v[1], v[3]), sub(v[1], v[3])
    turned = (d1[1], -d1[0]) if sign < 0 else (-d1[1], d1[0])
    return [add(s0, s1), add(d0, turned), sub(s0, s1), sub(d0, turned)]


def fourier16(v, sign):
    inner = [fourier4([v[4 * b1 + b0] for b1 in range(4)], sign) for b0 in range(4)]
    out = [None] * 16
    for q0 in range(4):
        column = []
        for b0 in range(4):
            angle = sign * 2.0 * math.pi * (b0 * q0) / 16
            factor = None if b0 * q0 == 0 else (math.cos(angle), math.sin(angle))
            column.append(times(inner[b0][q0], factor))
        for q1, value in enumerate(fourier4(column, sign)):
            out[q0 + 4 * q1] = value
    return out


def peer_of(j, gx, gy):
    k = lax.rem(j * STEP, PEERS)
    return lax.rem(gx + k // GY, GX), lax.rem(gy + lax.rem(k, GY), GY)


def kernel(
    one_ref, two_ref, depth_hi_ref, depth_lo_ref, tables_ref, factors_ref, out_ref,
    dens, depth_hi, depth_lo, tables, factors, twiddle, work, send, recv, send2, recv2, result,
    load_sem, table_sem, out_sem, send_sem, recv_sem, send2_sem, recv2_sem,
):
    gx = lax.axis_index("gx")
    gy = lax.axis_index("gy")
    me = gx * GY + gy

    barrier = pltpu.get_barrier_semaphore()

    @pl.loop(1, PEERS)
    def _(j):
        px, py = peer_of(j, gx, gy)
        pl.semaphore_signal(barrier, inc=1, device_id=(px, py), device_id_type=MESH)

    table_copies = [
        pltpu.make_async_copy(source, target, table_sem.at[i])
        for i, (source, target) in enumerate(
            (
                (depth_hi_ref, depth_hi),
                (depth_lo_ref, depth_lo),
                (tables_ref, tables),
                (factors_ref, factors),
            )
        )
    ]
    density_refs = (one_ref, two_ref)

    def density_copy(f, p):
        rows = pl.ds(p * 256, 256)
        return pltpu.make_async_copy(
            density_refs[f].at[rows], dens.at[f, rows], load_sem.at[f * 8 + p]
        )

    table_copies[0].start()
    table_copies[1].start()
    for f in range(2):
        for p in range(8):
            density_copy(f, p).start()
    table_copies[2].start()
    table_copies[3].start()
    table_copies[0].wait()
    table_copies[1].wait()

    def depth_forward(c):
        for f in range(2):
            @pl.loop(0, 8)
            def _(p):
                if c == 0:
                    density_copy(f, p).wait()
                cells = split(dens[f, pl.ds(p * 256, 256), :])
                lines = dot3((depth_hi[c], depth_lo[c]), cells, NT)
                for s in range(2):
                    for ri in range(2):
                        start = f * 32 + ri * 16 + 2 * p + s
                        send[c, pl.ds(start, PEERS, stride=FWD_PITCH), :] = lines[
                            ri * 128 : ri * 128 + 128, s * 128 : s * 128 + 128
                        ]

    def forward_sends(c):
        @pl.loop(1, PEERS)
        def _(j):
            px, py = peer_of(j, gx, gy)
            pltpu.make_async_remote_copy(
                src_ref=send.at[c, pl.ds((px * GY + py) * FWD_PITCH, FWD_ROWS)],
                dst_ref=recv.at[c, pl.ds(me * FWD_ROWS, FWD_ROWS)],
                send_sem=send_sem.at[c],
                recv_sem=recv_sem.at[c],
                device_id=(px, py),
                device_id_type=MESH,
            ).start()

        recv[c, pl.ds(me * FWD_ROWS, FWD_ROWS), :] = send[c, pl.ds(me * FWD_PITCH, FWD_ROWS), :]

    def back_sends(c):
        @pl.loop(1, PEERS)
        def _(j):
            px, py = peer_of(j, gx, gy)
            pltpu.make_async_remote_copy(
                src_ref=send2.at[c, pl.ds((px * GY + py) * BACK_ROWS, BACK_ROWS)],
                dst_ref=recv2.at[c, pl.ds(me * BACK_PITCH, BACK_ROWS)],
                send_sem=send2_sem.at[c],
                recv_sem=recv2_sem.at[c],
                device_id=(px, py),
                device_id_type=MESH,
            ).start()

        recv2[c, pl.ds(me * BACK_PITCH, BACK_ROWS), :] = send2[c, pl.ds(me * BACK_ROWS, BACK_ROWS), :]

    def forward_bytes(c, sem):
        rows = recv.at[c, pl.ds(0, (PEERS - 1) * FWD_ROWS)]
        pltpu.make_async_copy(rows, rows, sem.at[c]).wait()

    def back_bytes(c, sem):
        rows = send2.at[c, pl.ds(0, (PEERS - 1) * BACK_ROWS)]
        pltpu.make_async_copy(rows, rows, sem.at[c]).wait()

    def table(start, rows):
        return tables[start : start + rows, :], tables[start + rows : start + 2 * rows, :]

    def make_twiddles():
        @pl.loop(0, 16)
        def _(kb):
            x_re, x_im = factors[0:128, :], factors[128:256, :]
            y_re = factors[pl.ds(256 + kb, 1), :]
            y_im = factors[pl.ds(272 + kb, 1), :]
            twiddle[kb, 0:128, :] = x_re * y_re - x_im * y_im
            twiddle[kb, 128:256, :] = x_re * y_im + x_im * y_re

    def plane(c):
        for f in range(2):
            @pl.loop(0, 8)
            def _(pair):
                columns = []
                for s in range(2):
                    b = 2 * pair + s
                    blocks = [
                        recv[c, pl.ds((a * GY + b) * FWD_ROWS + f * 32 + ri * 16, 16), :]
                        for ri in range(2)
                        for a in range(GX)
                    ]
                    columns.append(jnp.concatenate(blocks, axis=0))
                lines = dot3(table(0, 256), split(jnp.concatenate(columns, axis=1)), NN)
                for s in range(2):
                    work[f, 2 * pair + s, :, :] = lines[:, s * 128 : s * 128 + 128]

            @pl.loop(0, 16)
            def _(k):
                re_rows = pl.ds(k * 8, 8)
                im_rows = pl.ds(128 + k * 8, 8)
                values = [(work[f, b, re_rows, :], work[f, b, im_rows, :]) for b in range(16)]
                for kb, value in enumerate(fourier16(values, -1)):
                    re, im = times(value, (twiddle[kb, re_rows, :], twiddle[kb, im_rows, :]))
                    work[f, kb, re_rows, :] = re
                    work[f, kb, im_rows, :] = im

        weight = jnp.where(me == 0, 1.0, 2.0) if c == 0 else 2.0
        scale = weight / float(SIDE**3)
        k1 = lax.broadcasted_iota(jnp.int32, (128, 128), 0)
        lane = lax.broadcasted_iota(jnp.int32, (128, 128), 1)
        keep_x = k1 + (lane // 32) * 128 != SIDE // 2

        @pl.loop(0, 16)
        def _(kb):
            keep = keep_x & (kb + lax.rem(lane, 32) * 16 != SIDE // 2)
            rows = [
                jnp.concatenate([work[f, kb, 0:128, :], work[f, kb, 128:256, :]], axis=1)
                for f in range(2)
            ]
            spectra = dot3(split(jnp.concatenate(rows, axis=0)), table(1024, 256), NN)
            product = (
                spectra[0:128, 0:128] * spectra[128:256, 0:128]
                + spectra[0:128, 128:256] * spectra[128:256, 128:256]
            )
            power = jnp.where(keep, product * scale, 0.0)
            lines = dot3(split(power), table(1536, 128), NN)
            t_re, t_im = twiddle[kb, 0:128, :], twiddle[kb, 128:256, :]
            re, im = lines[:, 0:128], lines[:, 128:256]
            work[0, kb, 0:128, :] = re * t_re + im * t_im
            work[0, kb, 128:256, :] = im * t_re - re * t_im

        @pl.loop(0, 16)
        def _(k):
            re_rows = pl.ds(k * 8, 8)
            im_rows = pl.ds(128 + k * 8, 8)
            values = [(work[0, kb, re_rows, :], work[0, kb, im_rows, :]) for kb in range(16)]
            for b, (re, im) in enumerate(fourier16(values, 1)):
                work[0, b, re_rows, :] = re
                work[0, b, im_rows, :] = im

        @pl.loop(0, 8)
        def _(pair):
            both = jnp.concatenate([work[0, 2 * pair], work[0, 2 * pair + 1]], axis=1)
            lines = dot3(table(512, 256), split(both), NN)
            for s in range(2):
                for a in range(GX):
                    for ri in range(2):
                        start = (a * GY + 2 * pair + s) * BACK_ROWS + ri * 16
                        send2[c, pl.ds(start, 16), :] = lines[
                            ri * 128 + a * 16 : ri * 128 + a * 16 + 16, s * 128 : s * 128 + 128
                        ]

    def out_copy(xt):
        rows = pl.ds(xt * 128, 128)
        return pltpu.make_async_copy(result.at[rows], out_ref.at[rows], out_sem.at[xt])

    def depth_inverse(c):
        @pl.loop(0, 16)
        def _(xt):
            lines = jnp.concatenate(
                [
                    recv2[c, pl.ds(ri * 16 + xt, PEERS, stride=BACK_PITCH), :].T
                    for ri in range(2)
                ],
                axis=1,
            )
            cells = dot3(split(lines), (depth_hi[c], depth_lo[c]), NN)
            rows = pl.ds(xt * 128, 128)
            if c == 0:
                result[rows, :] = cells
            else:
                result[rows, :] = (result[rows, :] + cells) * (SIDE**-1.5)
                out_copy(xt).start()

    depth_forward(0)
    pl.semaphore_wait(barrier, PEERS - 1)
    forward_sends(0)
    depth_forward(1)
    forward_sends(1)
    table_copies[2].wait()
    table_copies[3].wait()
    make_twiddles()
    for c in range(2):
        forward_bytes(c, recv_sem)
        plane(c)
        back_sends(c)
    for c in range(2):
        back_bytes(c, recv2_sem)
        depth_inverse(c)
    for c in range(2):
        forward_bytes(c, send_sem)
        back_bytes(c, send2_sem)

    @pl.loop(0, 16)
    def _(xt):
        out_copy(xt).wait()


def on_device(density_one, density_two):
    depth_hi, depth_lo = halves(depth_table())
    tables = plane_tables()
    factors = twiddle_factors()
    f32, bf16 = jnp.float32, jnp.bfloat16
    dma = pltpu.SemaphoreType.DMA
    rows = 2048
    out = pl.pallas_call(
        kernel,
        name="correlate",
        out_shape=jax.ShapeDtypeStruct((rows, SIDE), f32),
        in_specs=[pl.BlockSpec(memory_space=pl.ANY)] * 6,
        out_specs=pl.BlockSpec(memory_space=pl.ANY),
        scratch_shapes=[
            pltpu.VMEM((2, rows, SIDE), f32),
            pltpu.VMEM(depth_hi.shape, bf16),
            pltpu.VMEM(depth_lo.shape, bf16),
            pltpu.VMEM(tables.shape, bf16),
            pltpu.VMEM(factors.shape, f32),
            pltpu.VMEM((16, 256, 128), f32),
            pltpu.VMEM((2, 16, 256, 128), f32),
            pltpu.VMEM((2, PEERS * FWD_PITCH, 128), f32),
            pltpu.VMEM((2, PEERS * FWD_ROWS, 128), f32),
            pltpu.VMEM((2, PEERS * BACK_ROWS, 128), f32),
            pltpu.VMEM((2, PEERS * BACK_PITCH, 128), f32),
            pltpu.VMEM((rows, SIDE), f32),
            dma((16,)),
            dma((4,)),
            dma((16,)),
            dma((2,)),
            dma((2,)),
            dma((2,)),
            dma((2,)),
        ],
        compiler_params=pltpu.CompilerParams(
            collective_id=0, has_side_effects=True, vmem_limit_bytes=60 * 2**20
        ),
    )(
        density_one.reshape(rows, SIDE),
        density_two.reshape(rows, SIDE),
        jnp.asarray(depth_hi),
        jnp.asarray(depth_lo),
        jnp.asarray(tables),
        jnp.asarray(factors),
    )
    return out.reshape(density_one.shape)


def solution(mesh):
    return jax.shard_map(
        on_device,
        mesh=mesh,
        in_specs=(P("gx", "gy", None), P("gx", "gy", None)),
        out_specs=P("gx", "gy", None),
        check_vma=False,
    )
```

```python
import functools
import math

import jax
import jax.numpy as jnp
import ml_dtypes
import numpy as np
from jax import lax
from jax.experimental import pallas as pl
from jax.experimental.pallas import tpu as pltpu
from jax.sharding import PartitionSpec as P

MESH = pl.DeviceIdType.MESH
NT = (((1,), (1,)), ((), ()))
NN = (((1,), (0,)), ((), ()))

GX, GY = 8, 16
PEERS = GX * GY
SIDE = 512
FWD_ROWS = 32
FWD_PITCH = 40
BACK_ROWS = 32
BACK_PITCH = 40
STEP = 45


def halves(table):
    high = table.astype(np.float32).astype(ml_dtypes.bfloat16)
    low = (table - high.astype(np.float64)).astype(np.float32).astype(ml_dtypes.bfloat16)
    return high, low


def wave(numerator, length):
    angle = 2.0 * np.pi * (numerator % length) / length
    return np.cos(angle), np.sin(angle)


def depth_table():
    kz = np.arange(SIDE // 2).reshape(PEERS, 2).T
    cos, sin = wave(kz[:, :, None] * np.arange(SIDE // 2)[None, None, :], SIDE)
    return np.concatenate([cos, -sin], axis=1)


def plane_tables():
    m = np.arange(128)
    cos, sin = wave(m[:, None] * m[None, :], 128)
    rows_forward = np.block([[cos, sin], [-sin, cos]])
    rows_inverse = np.block([[cos, -sin], [sin, cos]])
    x4, y32 = m // 32, m % 32
    cos, sin = wave(
        128 * x4[:, None] * x4[None, :] + 16 * y32[:, None] * y32[None, :], SIDE
    )
    lanes_forward = np.block([[cos, -sin], [sin, cos]])
    lanes_inverse = np.concatenate([cos, sin], axis=1)
    parts = []
    for table in (rows_forward, rows_inverse, lanes_forward, lanes_inverse):
        parts.extend(halves(table))
    return np.concatenate(parts, axis=0)


def twiddle_factors():
    m = np.arange(128)
    x4, y32 = m // 32, m % 32
    x_cos, x_sin = wave(m[:, None] * x4[None, :], SIDE)
    y_cos, y_sin = wave(np.arange(16)[:, None] * y32[None, :], SIDE)
    return np.concatenate([x_cos, -x_sin, y_cos, -y_sin], axis=0).astype(np.float32)


def split(value):
    high = value.astype(jnp.bfloat16)
    low = (value - high.astype(jnp.float32)).astype(jnp.bfloat16)
    return high, low


def dot3(left, right, dims):
    def one(a, b):
        return lax.dot_general(a, b, dims, preferred_element_type=jnp.float32)

    return one(left[0], right[0]) + (one(left[0], right[1]) + one(left[1], right[0]))


def times(value, factor):
    if factor is None:
        return value
    (re, im), (c, s) = value, factor
    return (re * c - im * s, re * s + im * c)


def fourier4(v, sign):
    def add(p, q):
        return (p[0] + q[0], p[1] + q[1])

    def sub(p, q):
        return (p[0] - q[0], p[1] - q[1])

    s0, d0 = add(v[0], v[2]), sub(v[0], v[2])
    s1, d1 = add(v[1], v[3]), sub(v[1], v[3])
    turned = (d1[1], -d1[0]) if sign < 0 else (-d1[1], d1[0])
    return [add(s0, s1), add(d0, turned), sub(s0, s1), sub(d0, turned)]


def fourier16(v, sign):
    inner = [fourier4([v[4 * b1 + b0] for b1 in range(4)], sign) for b0 in range(4)]
    out = [None] * 16
    for q0 in range(4):
        column = []
        for b0 in range(4):
            angle = sign * 2.0 * math.pi * (b0 * q0) / 16
            factor = None if b0 * q0 == 0 else (math.cos(angle), math.sin(angle))
            column.append(times(inner[b0][q0], factor))
        for q1, value in enumerate(fourier4(column, sign)):
            out[q0 + 4 * q1] = value
    return out


def peer_of(j, gx, gy):
    k = lax.rem(j * STEP, PEERS)
    return lax.rem(gx + k // GY, GX), lax.rem(gy + lax.rem(k, GY), GY)


def kernel(
    one_ref, two_ref, depth_hi_ref, depth_lo_ref, tables_ref, factors_ref, out_ref,
    dens, depth_hi, depth_lo, tables, factors, twiddle, work, send, recv, send2, recv2, even, result,
    load_sem, table_sem, out_sem, send_sem, recv_sem, send2_sem, recv2_sem,
):
    gx = lax.axis_index("gx")
    gy = lax.axis_index("gy")
    me = gx * GY + gy

    table_copies = [
        pltpu.make_async_copy(source, target, table_sem.at[i])
        for i, (source, target) in enumerate(
            (
                (depth_hi_ref, depth_hi),
                (depth_lo_ref, depth_lo),
                (tables_ref, tables),
                (factors_ref, factors),
            )
        )
    ]
    density_refs = (one_ref, two_ref)

    def density_copy(f, p):
        rows = pl.ds(p * 256, 256)
        return pltpu.make_async_copy(
            density_refs[f].at[rows], dens.at[f, rows], load_sem.at[f * 8 + p]
        )

    table_copies[0].start()
    table_copies[1].start()
    for f in range(2):
        for p in range(8):
            density_copy(f, p).start()
    table_copies[2].start()
    table_copies[3].start()

    barrier = pltpu.get_barrier_semaphore()

    @pl.loop(1, PEERS)
    def _(j):
        px, py = peer_of(j, gx, gy)
        pl.semaphore_signal(barrier, inc=1, device_id=(px, py), device_id_type=MESH)

    table_copies[0].wait()
    table_copies[1].wait()

    def depth_forward(c, f):
        @pl.loop(0, 8)
        def _(p):
            if c == 0:
                density_copy(f, p).wait()
            rows = pl.ds(p * 256, 256)
            near, far = dens[f, rows, 0:256], dens[f, rows, 256:512]
            cells = split(near + far if c == 0 else near - far)
            lines = dot3((depth_hi[c], depth_lo[c]), cells, NT)
            for s in range(2):
                for ri in range(2):
                    start = ri * 16 + 2 * p + s
                    send[2 * c + f, pl.ds(start, PEERS, stride=FWD_PITCH), :] = lines[
                        ri * 128 : ri * 128 + 128, s * 128 : s * 128 + 128
                    ]

    def forward_sends(q):
        @pl.loop(1, PEERS)
        def _(j):
            px, py = peer_of(j, gx, gy)
            pltpu.make_async_remote_copy(
                src_ref=send.at[q, pl.ds((px * GY + py) * FWD_PITCH, FWD_ROWS)],
                dst_ref=recv.at[q, pl.ds(me * FWD_ROWS, FWD_ROWS)],
                send_sem=send_sem.at[q],
                recv_sem=recv_sem.at[q],
                device_id=(px, py),
                device_id_type=MESH,
            ).start()

        recv[q, pl.ds(me * FWD_ROWS, FWD_ROWS), :] = send[q, pl.ds(me * FWD_PITCH, FWD_ROWS), :]

    def back_sends(c):
        @pl.loop(1, PEERS)
        def _(j):
            px, py = peer_of(j, gx, gy)
            pltpu.make_async_remote_copy(
                src_ref=send2.at[c, pl.ds((px * GY + py) * BACK_ROWS, BACK_ROWS)],
                dst_ref=recv2.at[c, pl.ds(me * BACK_PITCH, BACK_ROWS)],
                send_sem=send2_sem.at[c],
                recv_sem=recv2_sem.at[c],
                device_id=(px, py),
                device_id_type=MESH,
            ).start()

        recv2[c, pl.ds(me * BACK_PITCH, BACK_ROWS), :] = send2[c, pl.ds(me * BACK_ROWS, BACK_ROWS), :]

    def forward_bytes(q, sem):
        rows = recv.at[q, pl.ds(0, (PEERS - 1) * FWD_ROWS)]
        pltpu.make_async_copy(rows, rows, sem.at[q]).wait()

    def back_bytes(c, sem):
        rows = send2.at[c, pl.ds(0, (PEERS - 1) * BACK_ROWS)]
        pltpu.make_async_copy(rows, rows, sem.at[c]).wait()

    def table(start, rows):
        return tables[start : start + rows, :], tables[start + rows : start + 2 * rows, :]

    def make_twiddles():
        @pl.loop(0, 16)
        def _(kb):
            x_re, x_im = factors[0:128, :], factors[128:256, :]
            y_re = factors[pl.ds(256 + kb, 1), :]
            y_im = factors[pl.ds(272 + kb, 1), :]
            twiddle[kb, 0:128, :] = x_re * y_re - x_im * y_im
            twiddle[kb, 128:256, :] = x_re * y_im + x_im * y_re

    def spectrum(c, f):
        @pl.loop(0, 8)
        def _(pair):
            columns = []
            for s in range(2):
                b = 2 * pair + s
                blocks = [
                    recv[2 * c + f, pl.ds((a * GY + b) * FWD_ROWS + ri * 16, 16), :]
                    for ri in range(2)
                    for a in range(GX)
                ]
                columns.append(jnp.concatenate(blocks, axis=0))
            lines = dot3(table(0, 256), split(jnp.concatenate(columns, axis=1)), NN)
            for s in range(2):
                work[f, 2 * pair + s, :, :] = lines[:, s * 128 : s * 128 + 128]

        @pl.loop(0, 16)
        def _(k):
            re_rows = pl.ds(k * 8, 8)
            im_rows = pl.ds(128 + k * 8, 8)
            values = [(work[f, b, re_rows, :], work[f, b, im_rows, :]) for b in range(16)]
            for kb, value in enumerate(fourier16(values, -1)):
                re, im = times(value, (twiddle[kb, re_rows, :], twiddle[kb, im_rows, :]))
                work[f, kb, re_rows, :] = re
                work[f, kb, im_rows, :] = im

    def correlate(c):
        weight = jnp.where(me == 0, 1.0, 2.0) if c == 0 else 2.0
        scale = weight / float(SIDE**3)
        k1 = lax.broadcasted_iota(jnp.int32, (128, 128), 0)
        lane = lax.broadcasted_iota(jnp.int32, (128, 128), 1)
        keep_x = k1 + (lane // 32) * 128 != SIDE // 2

        @pl.loop(0, 16)
        def _(kb):
            keep = keep_x & (kb + lax.rem(lane, 32) * 16 != SIDE // 2)
            rows = [
                jnp.concatenate([work[f, kb, 0:128, :], work[f, kb, 128:256, :]], axis=1)
                for f in range(2)
            ]
            spectra = dot3(split(jnp.concatenate(rows, axis=0)), table(1024, 256), NN)
            product = (
                spectra[0:128, 0:128] * spectra[128:256, 0:128]
                + spectra[0:128, 128:256] * spectra[128:256, 128:256]
            )
            power = jnp.where(keep, product * scale, 0.0)
            lines = dot3(split(power), table(1536, 128), NN)
            t_re, t_im = twiddle[kb, 0:128, :], twiddle[kb, 128:256, :]
            re, im = lines[:, 0:128], lines[:, 128:256]
            work[0, kb, 0:128, :] = re * t_re + im * t_im
            work[0, kb, 128:256, :] = im * t_re - re * t_im

        @pl.loop(0, 16)
        def _(k):
            re_rows = pl.ds(k * 8, 8)
            im_rows = pl.ds(128 + k * 8, 8)
            values = [(work[0, kb, re_rows, :], work[0, kb, im_rows, :]) for kb in range(16)]
            for b, (re, im) in enumerate(fourier16(values, 1)):
                work[0, b, re_rows, :] = re
                work[0, b, im_rows, :] = im

        @pl.loop(0, 8)
        def _(pair):
            both = jnp.concatenate([work[0, 2 * pair], work[0, 2 * pair + 1]], axis=1)
            lines = dot3(table(512, 256), split(both), NN)
            for s in range(2):
                for a in range(GX):
                    for ri in range(2):
                        start = (a * GY + 2 * pair + s) * BACK_ROWS + ri * 16
                        send2[c, pl.ds(start, 16), :] = lines[
                            ri * 128 + a * 16 : ri * 128 + a * 16 + 16, s * 128 : s * 128 + 128
                        ]

    def out_copy(p):
        rows = pl.ds(p * 256, 256)
        return pltpu.make_async_copy(result.at[rows], out_ref.at[rows], out_sem.at[p])

    def depth_inverse(c):
        @pl.loop(0, 8)
        def _(p):
            lines = jnp.concatenate(
                [
                    jnp.concatenate(
                        [
                            recv2[c, pl.ds(ri * 16 + 2 * p + s, PEERS, stride=BACK_PITCH), :].T
                            for ri in range(2)
                        ],
                        axis=1,
                    )
                    for s in range(2)
                ],
                axis=0,
            )
            cells = dot3(split(lines), (depth_hi[c], depth_lo[c]), NN)
            rows = pl.ds(p * 256, 256)
            if c == 0:
                even[rows, :] = cells
            else:
                result[rows, 0:256] = (even[rows, :] + cells) * (SIDE**-1.5)
                result[rows, 256:512] = (even[rows, :] - cells) * (SIDE**-1.5)
                out_copy(p).start()

    depth_forward(0, 0)
    pl.semaphore_wait(barrier, PEERS - 1)
    forward_sends(0)
    for q in range(1, 4):
        depth_forward(q // 2, q % 2)
        forward_sends(q)
    table_copies[2].wait()
    table_copies[3].wait()
    make_twiddles()
    for c in range(2):
        for f in range(2):
            forward_bytes(2 * c + f, recv_sem)
            if (c, f) == (1, 1):
                back_sends(0)
            spectrum(c, f)
        correlate(c)
    back_sends(1)
    for c in range(2):
        back_bytes(c, recv2_sem)
        depth_inverse(c)
    for q in range(4):
        forward_bytes(q, send_sem)
    for c in range(2):
        back_bytes(c, send2_sem)

    @pl.loop(0, 8)
    def _(p):
        out_copy(p).wait()


def on_device(density_one, density_two):
    depth_hi, depth_lo = halves(depth_table())
    tables = plane_tables()
    factors = twiddle_factors()
    f32, bf16 = jnp.float32, jnp.bfloat16
    dma = pltpu.SemaphoreType.DMA
    rows = 2048
    out = pl.pallas_call(
        kernel,
        name="correlate",
        out_shape=jax.ShapeDtypeStruct((rows, SIDE), f32),
        in_specs=[pl.BlockSpec(memory_space=pl.ANY)] * 6,
        out_specs=pl.BlockSpec(memory_space=pl.ANY),
        scratch_shapes=[
            pltpu.VMEM((2, rows, SIDE), f32),
            pltpu.VMEM(depth_hi.shape, bf16),
            pltpu.VMEM(depth_lo.shape, bf16),
            pltpu.VMEM(tables.shape, bf16),
            pltpu.VMEM(factors.shape, f32),
            pltpu.VMEM((16, 256, 128), f32),
            pltpu.VMEM((2, 16, 256, 128), f32),
            pltpu.VMEM((4, PEERS * FWD_PITCH, 128), f32),
            pltpu.VMEM((4, PEERS * FWD_ROWS, 128), f32),
            pltpu.VMEM((2, PEERS * BACK_ROWS, 128), f32),
            pltpu.VMEM((2, PEERS * BACK_PITCH, 128), f32),
            pltpu.VMEM((rows, SIDE // 2), f32),
            pltpu.VMEM((rows, SIDE), f32),
            dma((16,)),
            dma((4,)),
            dma((8,)),
            dma((4,)),
            dma((4,)),
            dma((2,)),
            dma((2,)),
        ],
        compiler_params=pltpu.CompilerParams(
            collective_id=0, has_side_effects=True, vmem_limit_bytes=60 * 2**20
        ),
    )(
        density_one.reshape(rows, SIDE),
        density_two.reshape(rows, SIDE),
        jnp.asarray(depth_hi),
        jnp.asarray(depth_lo),
        jnp.asarray(tables),
        jnp.asarray(factors),
    )
    return out.reshape(density_one.shape)


def solution(mesh):
    return jax.shard_map(
        on_device,
        mesh=mesh,
        in_specs=(P("gx", "gy", None), P("gx", "gy", None)),
        out_specs=P("gx", "gy", None),
        check_vma=False,
    )
```

```python
import functools
import math

import jax
import jax.numpy as jnp
from jax import lax
from jax.experimental import pallas as pl
from jax.experimental.pallas import tpu as pltpu
from jax.sharding import PartitionSpec as P

MESH = pl.DeviceIdType.MESH
NT = (((1,), (1,)), ((), ()))
NN = (((1,), (0,)), ((), ()))

GX, GY = 8, 16
PEERS = GX * GY
SIDE = 512
FWD_ROWS = 32
FWD_PITCH = 40
BACK_ROWS = 32
BACK_PITCH = 40
STEP = 45


def unit_cosine(numerator):
    folded = 128 - jnp.abs((numerator & (SIDE - 1)) - SIDE // 2)
    angle = folded.astype(jnp.float32) * (2.0 * math.pi / SIDE)
    square = angle * angle
    series = jnp.full_like(angle, -1.0 / math.factorial(11))
    for order in (9, 7, 5, 3, 1):
        sign = 1.0 if order % 4 == 1 else -1.0
        series = series * square + sign / math.factorial(order)
    return -(angle * series)


def split(value):
    high = value.astype(jnp.bfloat16)
    low = (value - high.astype(jnp.float32)).astype(jnp.bfloat16)
    return high, low


def dot3(left, right, dims):
    def one(a, b):
        return lax.dot_general(a, b, dims, preferred_element_type=jnp.float32)

    return one(left[0], right[0]) + (one(left[0], right[1]) + one(left[1], right[0]))


def times(value, factor):
    if factor is None:
        return value
    (re, im), (c, s) = value, factor
    return (re * c - im * s, re * s + im * c)


def fourier4(v, sign):
    def add(p, q):
        return (p[0] + q[0], p[1] + q[1])

    def sub(p, q):
        return (p[0] - q[0], p[1] - q[1])

    s0, d0 = add(v[0], v[2]), sub(v[0], v[2])
    s1, d1 = add(v[1], v[3]), sub(v[1], v[3])
    turned = (d1[1], -d1[0]) if sign < 0 else (-d1[1], d1[0])
    return [add(s0, s1), add(d0, turned), sub(s0, s1), sub(d0, turned)]


def fourier16(v, sign):
    inner = [fourier4([v[4 * b1 + b0] for b1 in range(4)], sign) for b0 in range(4)]
    out = [None] * 16
    for q0 in range(4):
        column = []
        for b0 in range(4):
            angle = sign * 2.0 * math.pi * (b0 * q0) / 16
            factor = None if b0 * q0 == 0 else (math.cos(angle), math.sin(angle))
            column.append(times(inner[b0][q0], factor))
        for q1, value in enumerate(fourier4(column, sign)):
            out[q0 + 4 * q1] = value
    return out


def peer_of(j, gx, gy):
    k = lax.rem(j * STEP, PEERS)
    return lax.rem(gx + k // GY, GX), lax.rem(gy + lax.rem(k, GY), GY)


def kernel(
    one_ref, two_ref, result,
    dens, tables, twiddle, work, send, recv, send2, recv2, even,
    load_sem, send_sem, recv_sem, send2_sem, recv2_sem,
):
    gx = lax.axis_index("gx")
    gy = lax.axis_index("gy")
    me = gx * GY + gy

    density_refs = (one_ref, two_ref)

    def density_copy(f, p):
        rows = pl.ds(p * 256, 256)
        return pltpu.make_async_copy(
            density_refs[f].at[rows], dens.at[f, rows], load_sem.at[f * 8 + p]
        )

    for f in range(2):
        for p in range(8):
            density_copy(f, p).start()

    barrier = pltpu.get_barrier_semaphore()

    @pl.loop(1, PEERS)
    def _(j):
        px, py = peer_of(j, gx, gy)
        pl.semaphore_signal(barrier, inc=1, device_id=(px, py), device_id_type=MESH)


    def table(start, rows):
        return tables[start : start + rows, :], tables[start + rows : start + 2 * rows, :]

    def fill(start, numerator):
        rows = numerator.shape[0]
        high, low = split(unit_cosine(numerator))
        tables[start : start + rows, :] = high
        tables[start + rows : start + 2 * rows, :] = low

    def grid(rows, columns):
        shape = (rows, columns)
        return (
            lax.broadcasted_iota(jnp.int32, shape, 0),
            lax.broadcasted_iota(jnp.int32, shape, 1),
        )

    def make_depth_table(c):
        row, cell = grid(256, 256)
        fill(c * 512, (2 * (row & 127) + c) * cell + (row & 128))

    def make_plane_tables():
        row, column = grid(256, 256)
        turn = (row & 128) - (column & 128)
        k, m = row & 127, column & 127
        fill(1024, 4 * k * m + turn)
        fill(1536, 4 * k * m - turn)
        lanes = 128 * (k >> 5) * (m >> 5) + 16 * (k & 31) * (m & 31)
        fill(2048, lanes - turn)
        row, column = grid(128, 256)
        m = column & 127
        fill(2560, 128 * (row >> 5) * (m >> 5) + 16 * (row & 31) * (m & 31) - (column & 128))

        @pl.loop(0, 16)
        def _(kb):
            row, lane = grid(256, 128)
            twiddle[kb, :, :] = unit_cosine(
                (lane >> 5) * (row & 127) + (lane & 31) * kb + (row & 128)
            )

    def depth_forward(c, f):
        @pl.loop(0, 8)
        def _(p):
            if c == 0:
                density_copy(f, p).wait()
            rows = pl.ds(p * 256, 256)
            near, far = dens[f, rows, 0:256], dens[f, rows, 256:512]
            cells = split(near + far if c == 0 else near - far)
            lines = dot3(table(c * 512, 256), cells, NT)
            for s in range(2):
                for ri in range(2):
                    start = ri * 16 + 2 * p + s
                    send[2 * c + f, pl.ds(start, PEERS, stride=FWD_PITCH), :] = lines[
                        ri * 128 : ri * 128 + 128, s * 128 : s * 128 + 128
                    ]

    def forward_sends(q):
        @pl.loop(1, PEERS)
        def _(j):
            px, py = peer_of(j, gx, gy)
            pltpu.make_async_remote_copy(
                src_ref=send.at[q, pl.ds((px * GY + py) * FWD_PITCH, FWD_ROWS)],
                dst_ref=recv.at[q, pl.ds(me * FWD_ROWS, FWD_ROWS)],
                send_sem=send_sem.at[q],
                recv_sem=recv_sem.at[q],
                device_id=(px, py),
                device_id_type=MESH,
            ).start()

        recv[q, pl.ds(me * FWD_ROWS, FWD_ROWS), :] = send[q, pl.ds(me * FWD_PITCH, FWD_ROWS), :]

    def back_sends(c):
        @pl.loop(1, PEERS)
        def _(j):
            px, py = peer_of(j, gx, gy)
            pltpu.make_async_remote_copy(
                src_ref=send2.at[c, pl.ds((px * GY + py) * BACK_ROWS, BACK_ROWS)],
                dst_ref=recv2.at[c, pl.ds(me * BACK_PITCH, BACK_ROWS)],
                send_sem=send2_sem.at[c],
                recv_sem=recv2_sem.at[c],
                device_id=(px, py),
                device_id_type=MESH,
            ).start()

        recv2[c, pl.ds(me * BACK_PITCH, BACK_ROWS), :] = send2[c, pl.ds(me * BACK_ROWS, BACK_ROWS), :]

    def forward_bytes(q, sem):
        rows = recv.at[q, pl.ds(0, (PEERS - 1) * FWD_ROWS)]
        pltpu.make_async_copy(rows, rows, sem.at[q]).wait()

    def back_bytes(c, sem):
        rows = send2.at[c, pl.ds(0, (PEERS - 1) * BACK_ROWS)]
        pltpu.make_async_copy(rows, rows, sem.at[c]).wait()

    def spectrum(c, f):
        @pl.loop(0, 8)
        def _(pair):
            columns = []
            for s in range(2):
                b = 2 * pair + s
                blocks = [
                    recv[2 * c + f, pl.ds((a * GY + b) * FWD_ROWS + ri * 16, 16), :]
                    for ri in range(2)
                    for a in range(GX)
                ]
                columns.append(jnp.concatenate(blocks, axis=0))
            lines = dot3(table(1024, 256), split(jnp.concatenate(columns, axis=1)), NN)
            for s in range(2):
                work[f, 2 * pair + s, :, :] = lines[:, s * 128 : s * 128 + 128]

        @pl.loop(0, 16)
        def _(k):
            re_rows = pl.ds(k * 8, 8)
            im_rows = pl.ds(128 + k * 8, 8)
            values = [(work[f, b, re_rows, :], work[f, b, im_rows, :]) for b in range(16)]
            for kb, value in enumerate(fourier16(values, -1)):
                re, im = times(value, (twiddle[kb, re_rows, :], twiddle[kb, im_rows, :]))
                work[f, kb, re_rows, :] = re
                work[f, kb, im_rows, :] = im

    def correlate(c):
        weight = jnp.where(me == 0, 1.0, 2.0) if c == 0 else 2.0
        scale = weight / float(SIDE**3)
        k1 = lax.broadcasted_iota(jnp.int32, (128, 128), 0)
        lane = lax.broadcasted_iota(jnp.int32, (128, 128), 1)
        keep_x = k1 + (lane // 32) * 128 != SIDE // 2

        @pl.loop(0, 16)
        def _(kb):
            keep = keep_x & (kb + lax.rem(lane, 32) * 16 != SIDE // 2)
            rows = [
                jnp.concatenate([work[f, kb, 0:128, :], work[f, kb, 128:256, :]], axis=1)
                for f in range(2)
            ]
            spectra = dot3(split(jnp.concatenate(rows, axis=0)), table(2048, 256), NN)
            product = (
                spectra[0:128, 0:128] * spectra[128:256, 0:128]
                + spectra[0:128, 128:256] * spectra[128:256, 128:256]
            )
            power = jnp.where(keep, product * scale, 0.0)
            lines = dot3(split(power), table(2560, 128), NN)
            t_re, t_im = twiddle[kb, 0:128, :], twiddle[kb, 128:256, :]
            re, im = lines[:, 0:128], lines[:, 128:256]
            work[0, kb, 0:128, :] = re * t_re + im * t_im
            work[0, kb, 128:256, :] = im * t_re - re * t_im

        @pl.loop(0, 16)
        def _(k):
            re_rows = pl.ds(k * 8, 8)
            im_rows = pl.ds(128 + k * 8, 8)
            values = [(work[0, kb, re_rows, :], work[0, kb, im_rows, :]) for kb in range(16)]
            for b, (re, im) in enumerate(fourier16(values, 1)):
                work[0, b, re_rows, :] = re
                work[0, b, im_rows, :] = im

        @pl.loop(0, 8)
        def _(pair):
            both = jnp.concatenate([work[0, 2 * pair], work[0, 2 * pair + 1]], axis=1)
            lines = dot3(table(1536, 256), split(both), NN)
            for s in range(2):
                for a in range(GX):
                    for ri in range(2):
                        start = (a * GY + 2 * pair + s) * BACK_ROWS + ri * 16
                        send2[c, pl.ds(start, 16), :] = lines[
                            ri * 128 + a * 16 : ri * 128 + a * 16 + 16, s * 128 : s * 128 + 128
                        ]

    def depth_inverse(c):
        @pl.loop(0, 8)
        def _(p):
            lines = jnp.concatenate(
                [
                    jnp.concatenate(
                        [
                            recv2[c, pl.ds(ri * 16 + 2 * p + s, PEERS, stride=BACK_PITCH), :].T
                            for ri in range(2)
                        ],
                        axis=1,
                    )
                    for s in range(2)
                ],
                axis=0,
            )
            cells = dot3(split(lines), table(c * 512, 256), NN)
            rows = pl.ds(p * 256, 256)
            if c == 0:
                even[rows, :] = cells
            else:
                result[rows, 0:256] = (even[rows, :] + cells) * (SIDE**-1.5)
                result[rows, 256:512] = (even[rows, :] - cells) * (SIDE**-1.5)

    make_depth_table(0)
    depth_forward(0, 0)
    pl.semaphore_wait(barrier, PEERS - 1)
    forward_sends(0)
    for q in range(1, 4):
        if q == 2:
            make_depth_table(1)
        depth_forward(q // 2, q % 2)
        forward_sends(q)
    make_plane_tables()
    for c in range(2):
        for f in range(2):
            if (c, f) == (1, 1):
                back_sends(0)
            forward_bytes(2 * c + f, recv_sem)
            spectrum(c, f)
        correlate(c)
    back_sends(1)
    for c in range(2):
        back_bytes(c, recv2_sem)
        depth_inverse(c)
    for q in range(4):
        forward_bytes(q, send_sem)
    for c in range(2):
        back_bytes(c, send2_sem)


def on_device(density_one, density_two):
    f32, bf16 = jnp.float32, jnp.bfloat16
    dma = pltpu.SemaphoreType.DMA
    rows = 2048
    out = pl.pallas_call(
        kernel,
        name="correlate",
        out_shape=jax.ShapeDtypeStruct((rows, SIDE), f32),
        in_specs=[pl.BlockSpec(memory_space=pltpu.HBM)] * 2,
        out_specs=pl.BlockSpec(memory_space=pltpu.VMEM),
        scratch_shapes=[
            pltpu.VMEM((2, rows, SIDE), f32),
            pltpu.VMEM((2816, 256), bf16),
            pltpu.VMEM((16, 256, 128), f32),
            pltpu.VMEM((2, 16, 256, 128), f32),
            pltpu.VMEM((4, PEERS * FWD_PITCH, 128), f32),
            pltpu.VMEM((4, PEERS * FWD_ROWS, 128), f32),
            pltpu.VMEM((2, PEERS * BACK_ROWS, 128), f32),
            pltpu.VMEM((2, PEERS * BACK_PITCH, 128), f32),
            pltpu.VMEM((rows, SIDE // 2), f32),
            dma((16,)),
            dma((4,)),
            dma((4,)),
            dma((2,)),
            dma((2,)),
        ],
        compiler_params=pltpu.CompilerParams(
            collective_id=0, has_side_effects=True, vmem_limit_bytes=48 * 2**20
        ),
    )(
        density_one.reshape(rows, SIDE),
        density_two.reshape(rows, SIDE),
    )
    return out.reshape(density_one.shape)


def solution(mesh):
    return jax.shard_map(
        on_device,
        mesh=mesh,
        in_specs=(P("gx", "gy", None), P("gx", "gy", None)),
        out_specs=P("gx", "gy", None),
        check_vma=False,
    )
```

```python
import functools
import math

import jax
import jax.numpy as jnp
from jax import lax
from jax.experimental import pallas as pl
from jax.experimental.pallas import tpu as pltpu
from jax.sharding import PartitionSpec as P

MESH = pl.DeviceIdType.MESH
NT = (((1,), (1,)), ((), ()))
NN = (((1,), (0,)), ((), ()))

GX, GY = 8, 16
PEERS = GX * GY
SIDE = 512
FWD_ROWS = 32
FWD_PITCH = 40
BACK_ROWS = 32
BACK_PITCH = 40
STEP = 45


def unit_cosine(numerator):
    folded = 128 - jnp.abs((numerator & (SIDE - 1)) - SIDE // 2)
    angle = folded.astype(jnp.float32) * (2.0 * math.pi / SIDE)
    square = angle * angle
    series = jnp.full_like(angle, -1.0 / math.factorial(11))
    for order in (9, 7, 5, 3, 1):
        sign = 1.0 if order % 4 == 1 else -1.0
        series = series * square + sign / math.factorial(order)
    return -(angle * series)


def split(value):
    high = value.astype(jnp.bfloat16)
    low = (value - high.astype(jnp.float32)).astype(jnp.bfloat16)
    return high, low


def dot3(left, right, dims):
    def one(a, b):
        return lax.dot_general(a, b, dims, preferred_element_type=jnp.float32)

    return one(left[0], right[0]) + (one(left[0], right[1]) + one(left[1], right[0]))


def times(value, factor):
    if factor is None:
        return value
    (re, im), (c, s) = value, factor
    return (re * c - im * s, re * s + im * c)


def fourier4(v, sign):
    def add(p, q):
        return (p[0] + q[0], p[1] + q[1])

    def sub(p, q):
        return (p[0] - q[0], p[1] - q[1])

    s0, d0 = add(v[0], v[2]), sub(v[0], v[2])
    s1, d1 = add(v[1], v[3]), sub(v[1], v[3])
    turned = (d1[1], -d1[0]) if sign < 0 else (-d1[1], d1[0])
    return [add(s0, s1), add(d0, turned), sub(s0, s1), sub(d0, turned)]


def fourier16(v, sign):
    inner = [fourier4([v[4 * b1 + b0] for b1 in range(4)], sign) for b0 in range(4)]
    out = [None] * 16
    for q0 in range(4):
        column = []
        for b0 in range(4):
            angle = sign * 2.0 * math.pi * (b0 * q0) / 16
            factor = None if b0 * q0 == 0 else (math.cos(angle), math.sin(angle))
            column.append(times(inner[b0][q0], factor))
        for q1, value in enumerate(fourier4(column, sign)):
            out[q0 + 4 * q1] = value
    return out


def far_first():
    def hops(offset):
        y, x = offset[0] % 4, offset[1] // 2 % 4
        return min(y, 4 - y) + min(x, 4 - x) + offset[0] // 4 + 2 * (offset[1] // 8)

    offsets = [(dx, dy) for dx in range(GX) for dy in range(GY) if dx or dy]
    return sorted(offsets, key=hops, reverse=True)


def peer_of(j, gx, gy):
    k = lax.rem(j * STEP, PEERS)
    return lax.rem(gx + k // GY, GX), lax.rem(gy + lax.rem(k, GY), GY)


def kernel(
    one_ref, two_ref, result,
    dens, tables, twiddle, work, send, recv, send2, recv2, even,
    load_sem, send_sem, recv_sem, send2_sem, recv2_sem,
):
    gx = lax.axis_index("gx")
    gy = lax.axis_index("gy")
    me = gx * GY + gy

    density_refs = (one_ref, two_ref)

    def density_copy(f, p):
        rows = pl.ds(p * 256, 256)
        return pltpu.make_async_copy(
            density_refs[f].at[rows], dens.at[f, rows], load_sem.at[f * 8 + p]
        )

    for f in range(2):
        for p in range(8):
            density_copy(f, p).start()

    barrier = pltpu.get_barrier_semaphore()

    columns_x = [lax.rem(gx + dx, GX) for dx in range(GX)]
    columns_y = [lax.rem(gy + dy, GY) for dy in range(GY)]
    for dx, dy in far_first():
        pl.semaphore_signal(
            barrier, inc=1, device_id=(columns_x[dx], columns_y[dy]), device_id_type=MESH
        )


    def table(start, rows):
        return tables[start : start + rows, :], tables[start + rows : start + 2 * rows, :]

    def fill(start, numerator):
        rows = numerator.shape[0]
        high, low = split(unit_cosine(numerator))
        tables[start : start + rows, :] = high
        tables[start + rows : start + 2 * rows, :] = low

    def grid(rows, columns):
        shape = (rows, columns)
        return (
            lax.broadcasted_iota(jnp.int32, shape, 0),
            lax.broadcasted_iota(jnp.int32, shape, 1),
        )

    def make_depth_table(c):
        row, cell = grid(256, 256)
        fill(c * 512, (2 * (row & 127) + c) * cell + (row & 128))

    def make_plane_tables():
        row, column = grid(256, 256)
        turn = (row & 128) - (column & 128)
        k, m = row & 127, column & 127
        fill(1024, 4 * k * m + turn)
        fill(1536, 4 * k * m - turn)
        lanes = 128 * (k >> 5) * (m >> 5) + 16 * (k & 31) * (m & 31)
        fill(2048, lanes - turn)
        row, column = grid(128, 256)
        m = column & 127
        fill(2560, 128 * (row >> 5) * (m >> 5) + 16 * (row & 31) * (m & 31) - (column & 128))

        @pl.loop(0, 16)
        def _(kb):
            row, lane = grid(256, 128)
            twiddle[kb, :, :] = unit_cosine(
                (lane >> 5) * (row & 127) + (lane & 31) * kb + (row & 128)
            )

    def depth_forward(c, f):
        @pl.loop(0, 8)
        def _(p):
            if c == 0:
                density_copy(f, p).wait()
            rows = pl.ds(p * 256, 256)
            near, far = dens[f, rows, 0:256], dens[f, rows, 256:512]
            cells = split(near + far if c == 0 else near - far)
            lines = dot3(table(c * 512, 256), cells, NT)
            for s in range(2):
                for ri in range(2):
                    start = ri * 16 + 2 * p + s
                    send[2 * c + f, pl.ds(start, PEERS, stride=FWD_PITCH), :] = lines[
                        ri * 128 : ri * 128 + 128, s * 128 : s * 128 + 128
                    ]

    def forward_sends(q):
        @pl.loop(1, PEERS)
        def _(j):
            px, py = peer_of(j, gx, gy)
            pltpu.make_async_remote_copy(
                src_ref=send.at[q, pl.ds((px * GY + py) * FWD_PITCH, FWD_ROWS)],
                dst_ref=recv.at[q, pl.ds(me * FWD_ROWS, FWD_ROWS)],
                send_sem=send_sem.at[q],
                recv_sem=recv_sem.at[q],
                device_id=(px, py),
                device_id_type=MESH,
            ).start()

        recv[q, pl.ds(me * FWD_ROWS, FWD_ROWS), :] = send[q, pl.ds(me * FWD_PITCH, FWD_ROWS), :]

    def back_sends(c):
        @pl.loop(1, PEERS)
        def _(j):
            px, py = peer_of(j, gx, gy)
            pltpu.make_async_remote_copy(
                src_ref=send2.at[c, pl.ds((px * GY + py) * BACK_ROWS, BACK_ROWS)],
                dst_ref=recv2.at[c, pl.ds(me * BACK_PITCH, BACK_ROWS)],
                send_sem=send2_sem.at[c],
                recv_sem=recv2_sem.at[c],
                device_id=(px, py),
                device_id_type=MESH,
            ).start()

        recv2[c, pl.ds(me * BACK_PITCH, BACK_ROWS), :] = send2[c, pl.ds(me * BACK_ROWS, BACK_ROWS), :]

    def forward_bytes(q, sem):
        rows = recv.at[q, pl.ds(0, (PEERS - 1) * FWD_ROWS)]
        pltpu.make_async_copy(rows, rows, sem.at[q]).wait()

    def back_bytes(c, sem):
        rows = send2.at[c, pl.ds(0, (PEERS - 1) * BACK_ROWS)]
        pltpu.make_async_copy(rows, rows, sem.at[c]).wait()

    def spectrum(c, f):
        @pl.loop(0, 8)
        def _(pair):
            columns = []
            for s in range(2):
                b = 2 * pair + s
                blocks = [
                    recv[2 * c + f, pl.ds((a * GY + b) * FWD_ROWS + ri * 16, 16), :]
                    for ri in range(2)
                    for a in range(GX)
                ]
                columns.append(jnp.concatenate(blocks, axis=0))
            lines = dot3(table(1024, 256), split(jnp.concatenate(columns, axis=1)), NN)
            for s in range(2):
                work[f, 2 * pair + s, :, :] = lines[:, s * 128 : s * 128 + 128]

        @pl.loop(0, 16)
        def _(k):
            re_rows = pl.ds(k * 8, 8)
            im_rows = pl.ds(128 + k * 8, 8)
            values = [(work[f, b, re_rows, :], work[f, b, im_rows, :]) for b in range(16)]
            for kb, value in enumerate(fourier16(values, -1)):
                re, im = times(value, (twiddle[kb, re_rows, :], twiddle[kb, im_rows, :]))
                work[f, kb, re_rows, :] = re
                work[f, kb, im_rows, :] = im

    def correlate(c):
        weight = jnp.where(me == 0, 1.0, 2.0) if c == 0 else 2.0
        scale = weight / float(SIDE**3)
        k1 = lax.broadcasted_iota(jnp.int32, (128, 128), 0)
        lane = lax.broadcasted_iota(jnp.int32, (128, 128), 1)
        keep_x = k1 + (lane // 32) * 128 != SIDE // 2

        @pl.loop(0, 16)
        def _(kb):
            keep = keep_x & (kb + lax.rem(lane, 32) * 16 != SIDE // 2)
            rows = [
                jnp.concatenate([work[f, kb, 0:128, :], work[f, kb, 128:256, :]], axis=1)
                for f in range(2)
            ]
            spectra = dot3(split(jnp.concatenate(rows, axis=0)), table(2048, 256), NN)
            product = (
                spectra[0:128, 0:128] * spectra[128:256, 0:128]
                + spectra[0:128, 128:256] * spectra[128:256, 128:256]
            )
            power = jnp.where(keep, product * scale, 0.0)
            lines = dot3(split(power), table(2560, 128), NN)
            t_re, t_im = twiddle[kb, 0:128, :], twiddle[kb, 128:256, :]
            re, im = lines[:, 0:128], lines[:, 128:256]
            work[0, kb, 0:128, :] = re * t_re + im * t_im
            work[0, kb, 128:256, :] = im * t_re - re * t_im

        @pl.loop(0, 16)
        def _(k):
            re_rows = pl.ds(k * 8, 8)
            im_rows = pl.ds(128 + k * 8, 8)
            values = [(work[0, kb, re_rows, :], work[0, kb, im_rows, :]) for kb in range(16)]
            for b, (re, im) in enumerate(fourier16(values, 1)):
                work[0, b, re_rows, :] = re
                work[0, b, im_rows, :] = im

        @pl.loop(0, 8)
        def _(pair):
            both = jnp.concatenate([work[0, 2 * pair], work[0, 2 * pair + 1]], axis=1)
            lines = dot3(table(1536, 256), split(both), NN)
            for s in range(2):
                for a in range(GX):
                    for ri in range(2):
                        start = (a * GY + 2 * pair + s) * BACK_ROWS + ri * 16
                        send2[c, pl.ds(start, 16), :] = lines[
                            ri * 128 + a * 16 : ri * 128 + a * 16 + 16, s * 128 : s * 128 + 128
                        ]

    def depth_inverse(c):
        @pl.loop(0, 8)
        def _(p):
            lines = jnp.concatenate(
                [
                    jnp.concatenate(
                        [
                            recv2[c, pl.ds(ri * 16 + 2 * p + s, PEERS, stride=BACK_PITCH), :].T
                            for ri in range(2)
                        ],
                        axis=1,
                    )
                    for s in range(2)
                ],
                axis=0,
            )
            cells = dot3(split(lines), table(c * 512, 256), NN)
            rows = pl.ds(p * 256, 256)
            if c == 0:
                even[rows, :] = cells
            else:
                result[rows, 0:256] = (even[rows, :] + cells) * (SIDE**-1.5)
                result[rows, 256:512] = (even[rows, :] - cells) * (SIDE**-1.5)

    make_depth_table(0)
    depth_forward(0, 0)
    pl.semaphore_wait(barrier, PEERS - 1)
    forward_sends(0)
    for q in range(1, 4):
        if q == 2:
            make_depth_table(1)
        depth_forward(q // 2, q % 2)
        forward_sends(q)
    make_plane_tables()
    for c in range(2):
        for f in range(2):
            if (c, f) == (1, 1):
                back_sends(0)
            forward_bytes(2 * c + f, recv_sem)
            spectrum(c, f)
        correlate(c)
    back_sends(1)
    for c in range(2):
        back_bytes(c, recv2_sem)
        depth_inverse(c)
    for q in range(4):
        forward_bytes(q, send_sem)
    for c in range(2):
        back_bytes(c, send2_sem)


def on_device(density_one, density_two):
    f32, bf16 = jnp.float32, jnp.bfloat16
    dma = pltpu.SemaphoreType.DMA
    rows = 2048
    out = pl.pallas_call(
        kernel,
        name="correlate",
        out_shape=jax.ShapeDtypeStruct((rows, SIDE), f32),
        in_specs=[pl.BlockSpec(memory_space=pltpu.HBM)] * 2,
        out_specs=pl.BlockSpec(memory_space=pltpu.VMEM),
        scratch_shapes=[
            pltpu.VMEM((2, rows, SIDE), f32),
            pltpu.VMEM((2816, 256), bf16),
            pltpu.VMEM((16, 256, 128), f32),
            pltpu.VMEM((2, 16, 256, 128), f32),
            pltpu.VMEM((4, PEERS * FWD_PITCH, 128), f32),
            pltpu.VMEM((4, PEERS * FWD_ROWS, 128), f32),
            pltpu.VMEM((2, PEERS * BACK_ROWS, 128), f32),
            pltpu.VMEM((2, PEERS * BACK_PITCH, 128), f32),
            pltpu.VMEM((rows, SIDE // 2), f32),
            dma((16,)),
            dma((4,)),
            dma((4,)),
            dma((2,)),
            dma((2,)),
        ],
        compiler_params=pltpu.CompilerParams(
            collective_id=0, has_side_effects=True, vmem_limit_bytes=48 * 2**20
        ),
    )(
        density_one.reshape(rows, SIDE),
        density_two.reshape(rows, SIDE),
    )
    return out.reshape(density_one.shape)


def solution(mesh):
    return jax.shard_map(
        on_device,
        mesh=mesh,
        in_specs=(P("gx", "gy", None), P("gx", "gy", None)),
        out_specs=P("gx", "gy", None),
        check_vma=False,
    )
```

```python
import functools
import math

import jax
import jax.numpy as jnp
from jax import lax
from jax.experimental import pallas as pl
from jax.experimental.pallas import tpu as pltpu
from jax.sharding import PartitionSpec as P

MESH = pl.DeviceIdType.MESH
NT = (((1,), (1,)), ((), ()))
NN = (((1,), (0,)), ((), ()))

GX, GY = 8, 16
PEERS = GX * GY
SIDE = 512
FWD_ROWS = 32
FWD_PITCH = 40
BACK_ROWS = 32
BACK_PITCH = 40
STEP = 45


def unit_cosine(numerator):
    folded = 128 - jnp.abs((numerator & (SIDE - 1)) - SIDE // 2)
    angle = folded.astype(jnp.float32) * (2.0 * math.pi / SIDE)
    square = angle * angle
    series = jnp.full_like(angle, -1.0 / math.factorial(11))
    for order in (9, 7, 5, 3, 1):
        sign = 1.0 if order % 4 == 1 else -1.0
        series = series * square + sign / math.factorial(order)
    return -(angle * series)


def split(value):
    high = value.astype(jnp.bfloat16)
    low = (value - high.astype(jnp.float32)).astype(jnp.bfloat16)
    return high, low


def dot3(left, right, dims):
    def one(a, b):
        return lax.dot_general(a, b, dims, preferred_element_type=jnp.float32)

    return one(left[0], right[0]) + (one(left[0], right[1]) + one(left[1], right[0]))


def times(value, factor):
    if factor is None:
        return value
    (re, im), (c, s) = value, factor
    return (re * c - im * s, re * s + im * c)


def fourier4(v, sign):
    def add(p, q):
        return (p[0] + q[0], p[1] + q[1])

    def sub(p, q):
        return (p[0] - q[0], p[1] - q[1])

    s0, d0 = add(v[0], v[2]), sub(v[0], v[2])
    s1, d1 = add(v[1], v[3]), sub(v[1], v[3])
    turned = (d1[1], -d1[0]) if sign < 0 else (-d1[1], d1[0])
    return [add(s0, s1), add(d0, turned), sub(s0, s1), sub(d0, turned)]


def fourier16(v, sign):
    inner = [fourier4([v[4 * b1 + b0] for b1 in range(4)], sign) for b0 in range(4)]
    out = [None] * 16
    for q0 in range(4):
        column = []
        for b0 in range(4):
            angle = sign * 2.0 * math.pi * (b0 * q0) / 16
            factor = None if b0 * q0 == 0 else (math.cos(angle), math.sin(angle))
            column.append(times(inner[b0][q0], factor))
        for q1, value in enumerate(fourier4(column, sign)):
            out[q0 + 4 * q1] = value
    return out


def far_first(most=12):
    def hops(offset):
        y, x = offset[0] % 4, offset[1] // 2 % 4
        near = min(y, 4 - y) + min(x, 4 - x) + offset[0] // 4 + 2 * (offset[1] // 8)
        return min(near, most)

    steps = [j * STEP % PEERS for j in range(1, PEERS)]
    offsets = [(k // GY, k % GY) for k in steps]
    return sorted(offsets, key=hops, reverse=True)


def peer_of(j, gx, gy):
    k = lax.rem(j * STEP, PEERS)
    return lax.rem(gx + k // GY, GX), lax.rem(gy + lax.rem(k, GY), GY)


def kernel(
    one_ref, two_ref, result,
    dens, tables, twiddle, work, send, recv, send2, recv2, even,
    load_sem, send_sem, recv_sem, send2_sem, recv2_sem,
):
    gx = lax.axis_index("gx")
    gy = lax.axis_index("gy")
    me = gx * GY + gy

    density_refs = (one_ref, two_ref)

    def density_copy(f, p):
        rows = pl.ds(p * 256, 256)
        return pltpu.make_async_copy(
            density_refs[f].at[rows], dens.at[f, rows], load_sem.at[f * 8 + p]
        )

    for f in range(2):
        for p in range(8):
            density_copy(f, p).start()

    barrier = pltpu.get_barrier_semaphore()

    columns_x = [lax.rem(gx + dx, GX) for dx in range(GX)]
    columns_y = [lax.rem(gy + dy, GY) for dy in range(GY)]
    for dx, dy in far_first():
        pl.semaphore_signal(
            barrier, inc=1, device_id=(columns_x[dx], columns_y[dy]), device_id_type=MESH
        )


    def table(start, rows):
        return tables[start : start + rows, :], tables[start + rows : start + 2 * rows, :]

    def fill(start, numerator):
        rows = numerator.shape[0]
        high, low = split(unit_cosine(numerator))
        tables[start : start + rows, :] = high
        tables[start + rows : start + 2 * rows, :] = low

    def grid(rows, columns):
        shape = (rows, columns)
        return (
            lax.broadcasted_iota(jnp.int32, shape, 0),
            lax.broadcasted_iota(jnp.int32, shape, 1),
        )

    def make_depth_table(c):
        row, cell = grid(256, 256)
        fill(c * 512, (2 * (row & 127) + c) * cell + (row & 128))

    def make_plane_tables():
        row, column = grid(256, 256)
        turn = (row & 128) - (column & 128)
        k, m = row & 127, column & 127
        fill(1024, 4 * k * m + turn)
        fill(1536, 4 * k * m - turn)
        lanes = 128 * (k >> 5) * (m >> 5) + 16 * (k & 31) * (m & 31)
        fill(2048, lanes - turn)
        row, column = grid(128, 256)
        m = column & 127
        fill(2560, 128 * (row >> 5) * (m >> 5) + 16 * (row & 31) * (m & 31) - (column & 128))

        @pl.loop(0, 16)
        def _(kb):
            row, lane = grid(256, 128)
            twiddle[kb, :, :] = unit_cosine(
                (lane >> 5) * (row & 127) + (lane & 31) * kb + (row & 128)
            )

    def depth_forward(c, f):
        @pl.loop(0, 8)
        def _(p):
            if c == 0:
                density_copy(f, p).wait()
            rows = pl.ds(p * 256, 256)
            near, far = dens[f, rows, 0:256], dens[f, rows, 256:512]
            cells = split(near + far if c == 0 else near - far)
            lines = dot3(table(c * 512, 256), cells, NT)
            for s in range(2):
                for ri in range(2):
                    start = ri * 16 + 2 * p + s
                    send[2 * c + f, pl.ds(start, PEERS, stride=FWD_PITCH), :] = lines[
                        ri * 128 : ri * 128 + 128, s * 128 : s * 128 + 128
                    ]

    def forward_sends(q):
        @pl.loop(1, PEERS)
        def _(j):
            px, py = peer_of(j, gx, gy)
            pltpu.make_async_remote_copy(
                src_ref=send.at[q, pl.ds((px * GY + py) * FWD_PITCH, FWD_ROWS)],
                dst_ref=recv.at[q, pl.ds(me * FWD_ROWS, FWD_ROWS)],
                send_sem=send_sem.at[q],
                recv_sem=recv_sem.at[q],
                device_id=(px, py),
                device_id_type=MESH,
            ).start()

        recv[q, pl.ds(me * FWD_ROWS, FWD_ROWS), :] = send[q, pl.ds(me * FWD_PITCH, FWD_ROWS), :]

    def back_sends(c):
        def to_peer(px, py):
            pltpu.make_async_remote_copy(
                src_ref=send2.at[c, pl.ds((px * GY + py) * BACK_ROWS, BACK_ROWS)],
                dst_ref=recv2.at[c, pl.ds(me * BACK_PITCH, BACK_ROWS)],
                send_sem=send2_sem.at[c],
                recv_sem=recv2_sem.at[c],
                device_id=(px, py),
                device_id_type=MESH,
            ).start()

        if c == 0:
            @pl.loop(1, PEERS)
            def _(j):
                to_peer(*peer_of(j, gx, gy))
        else:
            for dx, dy in far_first(2):
                to_peer(columns_x[dx], columns_y[dy])

        recv2[c, pl.ds(me * BACK_PITCH, BACK_ROWS), :] = send2[c, pl.ds(me * BACK_ROWS, BACK_ROWS), :]

    def forward_bytes(q, sem):
        rows = recv.at[q, pl.ds(0, (PEERS - 1) * FWD_ROWS)]
        pltpu.make_async_copy(rows, rows, sem.at[q]).wait()

    def back_bytes(c, sem):
        rows = send2.at[c, pl.ds(0, (PEERS - 1) * BACK_ROWS)]
        pltpu.make_async_copy(rows, rows, sem.at[c]).wait()

    def spectrum(c, f):
        @pl.loop(0, 8)
        def _(pair):
            columns = []
            for s in range(2):
                b = 2 * pair + s
                blocks = [
                    recv[2 * c + f, pl.ds((a * GY + b) * FWD_ROWS + ri * 16, 16), :]
                    for ri in range(2)
                    for a in range(GX)
                ]
                columns.append(jnp.concatenate(blocks, axis=0))
            lines = dot3(table(1024, 256), split(jnp.concatenate(columns, axis=1)), NN)
            for s in range(2):
                work[f, 2 * pair + s, :, :] = lines[:, s * 128 : s * 128 + 128]

        @pl.loop(0, 16)
        def _(k):
            re_rows = pl.ds(k * 8, 8)
            im_rows = pl.ds(128 + k * 8, 8)
            values = [(work[f, b, re_rows, :], work[f, b, im_rows, :]) for b in range(16)]
            for kb, value in enumerate(fourier16(values, -1)):
                re, im = times(value, (twiddle[kb, re_rows, :], twiddle[kb, im_rows, :]))
                work[f, kb, re_rows, :] = re
                work[f, kb, im_rows, :] = im

    def correlate(c):
        weight = jnp.where(me == 0, 1.0, 2.0) if c == 0 else 2.0
        scale = weight / float(SIDE**3)
        k1 = lax.broadcasted_iota(jnp.int32, (128, 128), 0)
        lane = lax.broadcasted_iota(jnp.int32, (128, 128), 1)
        keep_x = k1 + (lane // 32) * 128 != SIDE // 2

        @pl.loop(0, 16)
        def _(kb):
            keep = keep_x & (kb + lax.rem(lane, 32) * 16 != SIDE // 2)
            rows = [
                jnp.concatenate([work[f, kb, 0:128, :], work[f, kb, 128:256, :]], axis=1)
                for f in range(2)
            ]
            spectra = dot3(split(jnp.concatenate(rows, axis=0)), table(2048, 256), NN)
            product = (
                spectra[0:128, 0:128] * spectra[128:256, 0:128]
                + spectra[0:128, 128:256] * spectra[128:256, 128:256]
            )
            power = jnp.where(keep, product * scale, 0.0)
            lines = dot3(split(power), table(2560, 128), NN)
            t_re, t_im = twiddle[kb, 0:128, :], twiddle[kb, 128:256, :]
            re, im = lines[:, 0:128], lines[:, 128:256]
            work[0, kb, 0:128, :] = re * t_re + im * t_im
            work[0, kb, 128:256, :] = im * t_re - re * t_im

        @pl.loop(0, 16)
        def _(k):
            re_rows = pl.ds(k * 8, 8)
            im_rows = pl.ds(128 + k * 8, 8)
            values = [(work[0, kb, re_rows, :], work[0, kb, im_rows, :]) for kb in range(16)]
            for b, (re, im) in enumerate(fourier16(values, 1)):
                work[0, b, re_rows, :] = re
                work[0, b, im_rows, :] = im

        @pl.loop(0, 8)
        def _(pair):
            both = jnp.concatenate([work[0, 2 * pair], work[0, 2 * pair + 1]], axis=1)
            lines = dot3(table(1536, 256), split(both), NN)
            for s in range(2):
                for a in range(GX):
                    for ri in range(2):
                        start = (a * GY + 2 * pair + s) * BACK_ROWS + ri * 16
                        send2[c, pl.ds(start, 16), :] = lines[
                            ri * 128 + a * 16 : ri * 128 + a * 16 + 16, s * 128 : s * 128 + 128
                        ]

    def depth_inverse(c):
        @pl.loop(0, 8)
        def _(p):
            lines = jnp.concatenate(
                [
                    jnp.concatenate(
                        [
                            recv2[c, pl.ds(ri * 16 + 2 * p + s, PEERS, stride=BACK_PITCH), :].T
                            for ri in range(2)
                        ],
                        axis=1,
                    )
                    for s in range(2)
                ],
                axis=0,
            )
            cells = dot3(split(lines), table(c * 512, 256), NN)
            rows = pl.ds(p * 256, 256)
            if c == 0:
                even[rows, :] = cells
            else:
                result[rows, 0:256] = (even[rows, :] + cells) * (SIDE**-1.5)
                result[rows, 256:512] = (even[rows, :] - cells) * (SIDE**-1.5)

    make_depth_table(0)
    depth_forward(0, 0)
    pl.semaphore_wait(barrier, PEERS - 1)
    forward_sends(0)
    for q in range(1, 4):
        if q == 2:
            make_depth_table(1)
        depth_forward(q // 2, q % 2)
        forward_sends(q)
    make_plane_tables()
    for c in range(2):
        for f in range(2):
            if (c, f) == (1, 1):
                back_sends(0)
            forward_bytes(2 * c + f, recv_sem)
            spectrum(c, f)
        correlate(c)
    back_sends(1)
    for c in range(2):
        back_bytes(c, recv2_sem)
        depth_inverse(c)
    for q in range(4):
        forward_bytes(q, send_sem)
    for c in range(2):
        back_bytes(c, send2_sem)


def on_device(density_one, density_two):
    f32, bf16 = jnp.float32, jnp.bfloat16
    dma = pltpu.SemaphoreType.DMA
    rows = 2048
    out = pl.pallas_call(
        kernel,
        name="correlate",
        out_shape=jax.ShapeDtypeStruct((rows, SIDE), f32),
        in_specs=[pl.BlockSpec(memory_space=pltpu.HBM)] * 2,
        out_specs=pl.BlockSpec(memory_space=pltpu.VMEM),
        scratch_shapes=[
            pltpu.VMEM((2, rows, SIDE), f32),
            pltpu.VMEM((2816, 256), bf16),
            pltpu.VMEM((16, 256, 128), f32),
            pltpu.VMEM((2, 16, 256, 128), f32),
            pltpu.VMEM((4, PEERS * FWD_PITCH, 128), f32),
            pltpu.VMEM((4, PEERS * FWD_ROWS, 128), f32),
            pltpu.VMEM((2, PEERS * BACK_ROWS, 128), f32),
            pltpu.VMEM((2, PEERS * BACK_PITCH, 128), f32),
            pltpu.VMEM((rows, SIDE // 2), f32),
            dma((16,)),
            dma((4,)),
            dma((4,)),
            dma((2,)),
            dma((2,)),
        ],
        compiler_params=pltpu.CompilerParams(
            collective_id=0, has_side_effects=True, vmem_limit_bytes=48 * 2**20
        ),
    )(
        density_one.reshape(rows, SIDE),
        density_two.reshape(rows, SIDE),
    )
    return out.reshape(density_one.shape)


def solution(mesh):
    return jax.shard_map(
        on_device,
        mesh=mesh,
        in_specs=(P("gx", "gy", None), P("gx", "gy", None)),
        out_specs=P("gx", "gy", None),
        check_vma=False,
    )
```

```python
import functools
import math

import jax
import jax.numpy as jnp
from jax import lax
from jax.experimental import pallas as pl
from jax.experimental.pallas import tpu as pltpu
from jax.sharding import PartitionSpec as P

MESH = pl.DeviceIdType.MESH
NT = (((1,), (1,)), ((), ()))
NN = (((1,), (0,)), ((), ()))

GX, GY = 8, 16
PEERS = GX * GY
SIDE = 512
FWD_ROWS = 32
FWD_PITCH = 40
BACK_ROWS = 32
BACK_PITCH = 40
STEP = 45


def unit_cosine(numerator):
    folded = 128 - jnp.abs((numerator & (SIDE - 1)) - SIDE // 2)
    angle = folded.astype(jnp.float32) * (2.0 * math.pi / SIDE)
    square = angle * angle
    series = jnp.full_like(angle, -1.0 / math.factorial(11))
    for order in (9, 7, 5, 3, 1):
        sign = 1.0 if order % 4 == 1 else -1.0
        series = series * square + sign / math.factorial(order)
    return -(angle * series)


def split(value):
    high = value.astype(jnp.bfloat16)
    low = (value - high.astype(jnp.float32)).astype(jnp.bfloat16)
    return high, low


def dot3(left, right, dims):
    def one(a, b):
        return lax.dot_general(a, b, dims, preferred_element_type=jnp.float32)

    return one(left[0], right[0]) + (one(left[0], right[1]) + one(left[1], right[0]))


def times(value, factor):
    if factor is None:
        return value
    (re, im), (c, s) = value, factor
    return (re * c - im * s, re * s + im * c)


def fourier4(v, sign):
    def add(p, q):
        return (p[0] + q[0], p[1] + q[1])

    def sub(p, q):
        return (p[0] - q[0], p[1] - q[1])

    s0, d0 = add(v[0], v[2]), sub(v[0], v[2])
    s1, d1 = add(v[1], v[3]), sub(v[1], v[3])
    turned = (d1[1], -d1[0]) if sign < 0 else (-d1[1], d1[0])
    return [add(s0, s1), add(d0, turned), sub(s0, s1), sub(d0, turned)]


def fourier16(v, sign):
    inner = [fourier4([v[4 * b1 + b0] for b1 in range(4)], sign) for b0 in range(4)]
    out = [None] * 16
    for q0 in range(4):
        column = []
        for b0 in range(4):
            angle = sign * 2.0 * math.pi * (b0 * q0) / 16
            factor = None if b0 * q0 == 0 else (math.cos(angle), math.sin(angle))
            column.append(times(inner[b0][q0], factor))
        for q1, value in enumerate(fourier4(column, sign)):
            out[q0 + 4 * q1] = value
    return out


def far_first(most=12):
    def hops(offset):
        y, x = offset[0] % 4, offset[1] // 2 % 4
        z = offset[0] // 4 + 2 * (offset[1] // 8)
        near = min(y, 4 - y) + min(x, 4 - x) + min(z, 4 - z)
        return min(near, most)

    steps = [j * STEP % PEERS for j in range(1, PEERS)]
    offsets = [(k // GY, k % GY) for k in steps]
    return sorted(offsets, key=hops, reverse=True)


def peer_of(j, gx, gy):
    k = lax.rem(j * STEP, PEERS)
    return lax.rem(gx + k // GY, GX), lax.rem(gy + lax.rem(k, GY), GY)


def kernel(
    one_ref, two_ref, result,
    dens, tables, twiddle, work, send, recv, send2, recv2, even,
    load_sem, send_sem, recv_sem, send2_sem, recv2_sem,
):
    gx = lax.axis_index("gx")
    gy = lax.axis_index("gy")
    me = gx * GY + gy

    density_refs = (one_ref, two_ref)

    def density_copy(f, p):
        rows = pl.ds(p * 256, 256)
        return pltpu.make_async_copy(
            density_refs[f].at[rows], dens.at[f, rows], load_sem.at[f * 8 + p]
        )

    for f in range(2):
        for p in range(8):
            density_copy(f, p).start()

    barrier = pltpu.get_barrier_semaphore()

    columns_x = [lax.rem(gx + dx, GX) for dx in range(GX)]
    columns_y = [lax.rem(gy + dy, GY) for dy in range(GY)]
    for dx, dy in far_first():
        pl.semaphore_signal(
            barrier, inc=1, device_id=(columns_x[dx], columns_y[dy]), device_id_type=MESH
        )


    def table(start, rows):
        return tables[start : start + rows, :], tables[start + rows : start + 2 * rows, :]

    def fill(start, numerator):
        rows = numerator.shape[0]
        high, low = split(unit_cosine(numerator))
        tables[start : start + rows, :] = high
        tables[start + rows : start + 2 * rows, :] = low

    def grid(rows, columns):
        shape = (rows, columns)
        return (
            lax.broadcasted_iota(jnp.int32, shape, 0),
            lax.broadcasted_iota(jnp.int32, shape, 1),
        )

    def make_depth_table(c):
        row, cell = grid(256, 256)
        fill(c * 512, (2 * (row & 127) + c) * cell + (row & 128))

    def make_plane_tables():
        row, column = grid(256, 256)
        turn = (row & 128) - (column & 128)
        k, m = row & 127, column & 127
        fill(1024, 4 * k * m + turn)
        fill(1536, 4 * k * m - turn)
        lanes = 128 * (k >> 5) * (m >> 5) + 16 * (k & 31) * (m & 31)
        fill(2048, lanes - turn)
        row, column = grid(128, 256)
        m = column & 127
        fill(2560, 128 * (row >> 5) * (m >> 5) + 16 * (row & 31) * (m & 31) - (column & 128))

        @pl.loop(0, 16)
        def _(kb):
            row, lane = grid(256, 128)
            twiddle[kb, :, :] = unit_cosine(
                (lane >> 5) * (row & 127) + (lane & 31) * kb + (row & 128)
            )

    def depth_forward(c, f):
        @pl.loop(0, 8)
        def _(p):
            if c == 0:
                density_copy(f, p).wait()
            rows = pl.ds(p * 256, 256)
            near, far = dens[f, rows, 0:256], dens[f, rows, 256:512]
            cells = split(near + far if c == 0 else near - far)
            lines = dot3(table(c * 512, 256), cells, NT)
            for s in range(2):
                for ri in range(2):
                    start = ri * 16 + 2 * p + s
                    send[2 * c + f, pl.ds(start, PEERS, stride=FWD_PITCH), :] = lines[
                        ri * 128 : ri * 128 + 128, s * 128 : s * 128 + 128
                    ]

    def forward_sends(q):
        @pl.loop(1, PEERS)
        def _(j):
            px, py = peer_of(j, gx, gy)
            pltpu.make_async_remote_copy(
                src_ref=send.at[q, pl.ds((px * GY + py) * FWD_PITCH, FWD_ROWS)],
                dst_ref=recv.at[q, pl.ds(me * FWD_ROWS, FWD_ROWS)],
                send_sem=send_sem.at[q],
                recv_sem=recv_sem.at[q],
                device_id=(px, py),
                device_id_type=MESH,
            ).start()

        recv[q, pl.ds(me * FWD_ROWS, FWD_ROWS), :] = send[q, pl.ds(me * FWD_PITCH, FWD_ROWS), :]

    def back_sends(c):
        def to_peer(px, py):
            pltpu.make_async_remote_copy(
                src_ref=send2.at[c, pl.ds((px * GY + py) * BACK_ROWS, BACK_ROWS)],
                dst_ref=recv2.at[c, pl.ds(me * BACK_PITCH, BACK_ROWS)],
                send_sem=send2_sem.at[c],
                recv_sem=recv2_sem.at[c],
                device_id=(px, py),
                device_id_type=MESH,
            ).start()

        if c == 0:
            @pl.loop(1, PEERS)
            def _(j):
                to_peer(*peer_of(j, gx, gy))
        else:
            for dx, dy in far_first(2):
                to_peer(columns_x[dx], columns_y[dy])

        recv2[c, pl.ds(me * BACK_PITCH, BACK_ROWS), :] = send2[c, pl.ds(me * BACK_ROWS, BACK_ROWS), :]

    def forward_bytes(q, sem):
        rows = recv.at[q, pl.ds(0, (PEERS - 1) * FWD_ROWS)]
        pltpu.make_async_copy(rows, rows, sem.at[q]).wait()

    def back_bytes(c, sem):
        rows = send2.at[c, pl.ds(0, (PEERS - 1) * BACK_ROWS)]
        pltpu.make_async_copy(rows, rows, sem.at[c]).wait()

    def spectrum(c, f):
        @pl.loop(0, 8)
        def _(pair):
            columns = []
            for s in range(2):
                b = 2 * pair + s
                blocks = [
                    recv[2 * c + f, pl.ds((a * GY + b) * FWD_ROWS + ri * 16, 16), :]
                    for ri in range(2)
                    for a in range(GX)
                ]
                columns.append(jnp.concatenate(blocks, axis=0))
            lines = dot3(table(1024, 256), split(jnp.concatenate(columns, axis=1)), NN)
            for s in range(2):
                work[f, 2 * pair + s, :, :] = lines[:, s * 128 : s * 128 + 128]

        @pl.loop(0, 16)
        def _(k):
            re_rows = pl.ds(k * 8, 8)
            im_rows = pl.ds(128 + k * 8, 8)
            values = [(work[f, b, re_rows, :], work[f, b, im_rows, :]) for b in range(16)]
            for kb, value in enumerate(fourier16(values, -1)):
                re, im = times(value, (twiddle[kb, re_rows, :], twiddle[kb, im_rows, :]))
                work[f, kb, re_rows, :] = re
                work[f, kb, im_rows, :] = im

    def correlate(c):
        weight = jnp.where(me == 0, 1.0, 2.0) if c == 0 else 2.0
        scale = weight / float(SIDE**3)
        k1 = lax.broadcasted_iota(jnp.int32, (128, 128), 0)
        lane = lax.broadcasted_iota(jnp.int32, (128, 128), 1)
        keep_x = k1 + (lane // 32) * 128 != SIDE // 2

        @pl.loop(0, 16)
        def _(kb):
            keep = keep_x & (kb + lax.rem(lane, 32) * 16 != SIDE // 2)
            rows = [
                jnp.concatenate([work[f, kb, 0:128, :], work[f, kb, 128:256, :]], axis=1)
                for f in range(2)
            ]
            spectra = dot3(split(jnp.concatenate(rows, axis=0)), table(2048, 256), NN)
            product = (
                spectra[0:128, 0:128] * spectra[128:256, 0:128]
                + spectra[0:128, 128:256] * spectra[128:256, 128:256]
            )
            power = jnp.where(keep, product * scale, 0.0)
            lines = dot3(split(power), table(2560, 128), NN)
            t_re, t_im = twiddle[kb, 0:128, :], twiddle[kb, 128:256, :]
            re, im = lines[:, 0:128], lines[:, 128:256]
            work[0, kb, 0:128, :] = re * t_re + im * t_im
            work[0, kb, 128:256, :] = im * t_re - re * t_im

        @pl.loop(0, 16)
        def _(k):
            re_rows = pl.ds(k * 8, 8)
            im_rows = pl.ds(128 + k * 8, 8)
            values = [(work[0, kb, re_rows, :], work[0, kb, im_rows, :]) for kb in range(16)]
            for b, (re, im) in enumerate(fourier16(values, 1)):
                work[0, b, re_rows, :] = re
                work[0, b, im_rows, :] = im

        @pl.loop(0, 8)
        def _(pair):
            both = jnp.concatenate([work[0, 2 * pair], work[0, 2 * pair + 1]], axis=1)
            lines = dot3(table(1536, 256), split(both), NN)
            for s in range(2):
                for a in range(GX):
                    for ri in range(2):
                        start = (a * GY + 2 * pair + s) * BACK_ROWS + ri * 16
                        send2[c, pl.ds(start, 16), :] = lines[
                            ri * 128 + a * 16 : ri * 128 + a * 16 + 16, s * 128 : s * 128 + 128
                        ]

    def depth_inverse(c):
        @pl.loop(0, 8)
        def _(p):
            lines = jnp.concatenate(
                [
                    jnp.concatenate(
                        [
                            recv2[c, pl.ds(ri * 16 + 2 * p + s, PEERS, stride=BACK_PITCH), :].T
                            for ri in range(2)
                        ],
                        axis=1,
                    )
                    for s in range(2)
                ],
                axis=0,
            )
            cells = dot3(split(lines), table(c * 512, 256), NN)
            rows = pl.ds(p * 256, 256)
            if c == 0:
                even[rows, :] = cells
            else:
                result[rows, 0:256] = (even[rows, :] + cells) * (SIDE**-1.5)
                result[rows, 256:512] = (even[rows, :] - cells) * (SIDE**-1.5)

    make_depth_table(0)
    depth_forward(0, 0)
    pl.semaphore_wait(barrier, PEERS - 1)
    forward_sends(0)
    for q in range(1, 4):
        if q == 2:
            make_depth_table(1)
        depth_forward(q // 2, q % 2)
        forward_sends(q)
    make_plane_tables()
    for c in range(2):
        for f in range(2):
            if (c, f) == (1, 1):
                back_sends(0)
            forward_bytes(2 * c + f, recv_sem)
            spectrum(c, f)
        correlate(c)
    back_sends(1)
    for c in range(2):
        back_bytes(c, recv2_sem)
        depth_inverse(c)
    for q in range(4):
        forward_bytes(q, send_sem)
    for c in range(2):
        back_bytes(c, send2_sem)


def on_device(density_one, density_two):
    f32, bf16 = jnp.float32, jnp.bfloat16
    dma = pltpu.SemaphoreType.DMA
    rows = 2048
    out = pl.pallas_call(
        kernel,
        name="correlate",
        out_shape=jax.ShapeDtypeStruct((rows, SIDE), f32),
        in_specs=[pl.BlockSpec(memory_space=pltpu.HBM)] * 2,
        out_specs=pl.BlockSpec(memory_space=pltpu.VMEM),
        scratch_shapes=[
            pltpu.VMEM((2, rows, SIDE), f32),
            pltpu.VMEM((2816, 256), bf16),
            pltpu.VMEM((16, 256, 128), f32),
            pltpu.VMEM((2, 16, 256, 128), f32),
            pltpu.VMEM((4, PEERS * FWD_PITCH, 128), f32),
            pltpu.VMEM((4, PEERS * FWD_ROWS, 128), f32),
            pltpu.VMEM((2, PEERS * BACK_ROWS, 128), f32),
            pltpu.VMEM((2, PEERS * BACK_PITCH, 128), f32),
            pltpu.VMEM((rows, SIDE // 2), f32),
            dma((16,)),
            dma((4,)),
            dma((4,)),
            dma((2,)),
            dma((2,)),
        ],
        compiler_params=pltpu.CompilerParams(
            collective_id=0, has_side_effects=True, vmem_limit_bytes=48 * 2**20
        ),
    )(
        density_one.reshape(rows, SIDE),
        density_two.reshape(rows, SIDE),
    )
    return out.reshape(density_one.shape)


def solution(mesh):
    return jax.shard_map(
        on_device,
        mesh=mesh,
        in_specs=(P("gx", "gy", None), P("gx", "gy", None)),
        out_specs=P("gx", "gy", None),
        check_vma=False,
    )
```
